32 devices in a mesh: section: 4 (over z), node: 4 (over x, core), local: 2 (over y).
Axes of the slice: x: 2, y: 2, z: 4, core: 2. Of those that a mesh axis runs over, the one named last changes fastest.
Arguments:
- tokens: bfloat16 [4, 768, 7168], P('section', ('node', 'local')), may hold values from -6 to 6
- routes: int32 [4, 768, 8], P('section', ('node', 'local')), may hold values from 0 to 383, as said below
- route_gates: float32 [4, 768, 8], P('section', ('node', 'local')), may hold values from 0.2 to 1
- replica_table: int32 [4], replicated, may hold values from 0 to 2, as said below
- w_gate: bfloat16 [4, 7168, 256], P('node', None, 'local')
- w_up: bfloat16 [4, 7168, 256], P('node', None, 'local')
- w_down: bfloat16 [4, 256, 7168], P('node', 'local')
Outputs:
- section_input: bfloat16 [4, 768, 7168], P('section', ('node', 'local'))
The draws below stay inside these ranges and needn't reach their ends.
Inputs may be any that keep to these rules, and one draw needn't show every extreme that they name: `replica_table`: each of the experts 0 to 2 is held by one or two slots; slots that hold the same expert hold equal weights in w_gate, w_up and w_down. `routes`: each row names 8 different experts. Within the rows of one device, expert e < 3 is named by at least one row and by at most 2 times its number of slots in replica_table; in every draw some expert with one slot is named by exactly 2 rows of every device.
All inputs are finite; a program needn't handle non-finite values.
Results may differ from the reference program's by a relative error of at most 0.015.
Values may be sent and summed in bfloat16 or wider, within the bound.
A program may use at most 64 MiB of HBM per device.

```python
import jax
import jax.numpy as jnp
from jax import lax

D = 7168
ROUTED_EXPERTS = 384
TOPK = 8
HID_DEV = 128
CAP = 2
TOK_DEV = 96
FFW = 256
EXPERTS_AFLOAT = 3
TOKG = 768
N_SECTION = 4
N_NODE = 4
N_LOCAL = 2


def replica_table_of(key):
    table_key = jax.random.fold_in(key, 7001)
    extra = N_NODE - EXPERTS_AFLOAT
    hot_experts = jax.random.permutation(jax.random.fold_in(table_key, 1), EXPERTS_AFLOAT)[:extra]
    slots = jnp.concatenate([jnp.arange(EXPERTS_AFLOAT, dtype=jnp.int32), hot_experts.astype(jnp.int32)])
    return jax.random.permutation(jax.random.fold_in(table_key, 2), slots).astype(jnp.int32)


def draw_replica_table(key, part):
    return replica_table_of(key)


def draw_routes(key, part):
    slot_table = replica_table_of(key)
    route_key = jax.random.fold_in(key, 7002)
    blocks = N_SECTION * N_NODE * N_LOCAL
    expert_ids = jnp.arange(EXPERTS_AFLOAT, dtype=jnp.int32)
    copies = jnp.sum((slot_table[None, :] == expert_ids[:, None]).astype(jnp.int32), axis=1)
    most_rows = CAP * copies
    loads = jax.random.randint(jax.random.fold_in(route_key, 1), (blocks, EXPERTS_AFLOAT), 1, most_rows[None, :] + 1)
    full_expert = jnp.argmax(copies == 1).astype(jnp.int32)
    loads = jnp.where(expert_ids[None, :] == full_expert, CAP, loads)
    order_keys = jax.random.split(jax.random.fold_in(route_key, 2), blocks * EXPERTS_AFLOAT)
    ranks = jax.vmap(lambda one_key: jnp.argsort(jax.random.permutation(one_key, TOK_DEV)))(order_keys)
    ranks = ranks.reshape(blocks, EXPERTS_AFLOAT, TOK_DEV)
    labeled_flag = ranks < loads[:, :, None]
    labeled_flag = jnp.transpose(labeled_flag, (0, 2, 1)).reshape(blocks * TOK_DEV, EXPERTS_AFLOAT)
    row_total = blocks * TOK_DEV
    noise = jax.random.randint(jax.random.fold_in(route_key, 3), (row_total, ROUTED_EXPERTS), 0, 1 << 20)
    every_expert_index = jnp.arange(ROUTED_EXPERTS, dtype=jnp.int32)
    router_logit = noise * 512 + every_expert_index[None, :]
    traveling_piece = jnp.pad(labeled_flag, ((0, 0), (0, ROUTED_EXPERTS - EXPERTS_AFLOAT)))
    router_logit = jnp.where(every_expert_index[None, :] < EXPERTS_AFLOAT, jnp.where(traveling_piece, router_logit + (1 << 29), -1), router_logit)
    unused, chosen = lax.top_k(router_logit, TOPK)
    return chosen.astype(jnp.int32).reshape(N_SECTION, TOKG, TOPK)


def slot_weights(key, salt, array_shape, fan_in):
    slot_table = replica_table_of(key)
    weight_key = jax.random.fold_in(key, salt)

    def one_slot(expert):
        return jax.random.normal(jax.random.fold_in(weight_key, expert), array_shape, jnp.float32) * fan_in ** (-0.5)
    return jax.vmap(one_slot)(slot_table).astype(jnp.bfloat16)


def draw_w_gate(key, part):
    return slot_weights(key, 7003, (D, FFW), D)


def draw_w_up(key, part):
    return slot_weights(key, 7004, (D, FFW), D)


def draw_w_down(key, part):
    return slot_weights(key, 7005, (FFW, D), FFW)


def levels(own_key, dims, cuts, least, largest):
    loudness = 1.0
    for position, shards_of in cuts:
        steps = jax.random.uniform(jax.random.fold_in(jax.random.fold_in(own_key, 6), position), (shards_of,), jnp.float32, least / len(cuts), largest / len(cuts))
        loudness = loudness * jnp.repeat(jnp.exp(steps), dims[position] // shards_of).reshape((-1,) + (1,) * (len(dims) - 1 - position))
    return loudness


def normal_values(stream_key, extent, deviation, limit, cuts=(), held_as=jnp.bfloat16):
    array = jax.random.normal(stream_key, extent, jnp.float32) * deviation
    if len(cuts) > 0:
        array = levels(stream_key, extent, cuts, -0.22, 0.18) * array
    return jnp.clip(array, min=-limit, max=limit).astype(held_as)


def setup_inputs(seed: int = 0) -> dict:
    arg_keys = jax.random.split(jax.random.key(seed), 8)
    tokens = normal_values(arg_keys[0], (N_SECTION, TOKG, D), 1.0, 6.0, ((0, 4), (1, 8)))
    routes = draw_routes(jax.random.fold_in(arg_keys[7], 71), 0)
    route_gates = jnp.clip(0.2 + 0.8 * jax.random.uniform(arg_keys[2], (N_SECTION, TOKG, TOPK), jnp.float32) ** levels(arg_keys[2], (N_SECTION, TOKG, TOPK), ((0, 4), (1, 8)), -0.2, 0.2), 0.2, 1.0)
    replica_table = draw_replica_table(jax.random.fold_in(arg_keys[7], 71), 0)
    w_gate = draw_w_gate(jax.random.fold_in(arg_keys[7], 71), 0)
    w_up = draw_w_up(jax.random.fold_in(arg_keys[7], 71), 0)
    w_down = draw_w_down(jax.random.fold_in(arg_keys[7], 71), 0)
    return dict(tokens=tokens, routes=routes, route_gates=route_gates, replica_table=replica_table, w_gate=w_gate, w_up=w_up, w_down=w_down)


def reference(tokens, routes, route_gates, replica_table, w_gate, w_up, w_down):
    most_rows = N_NODE * N_LOCAL * 2 * CAP
    row_total = tokens.shape[1]

    def one_section(section_args):
        section_rows, pick_ids, gate_vals = section_args
        accum_out = jnp.zeros((row_total, D), jnp.float32)
        for expert in range(EXPERTS_AFLOAT):
            slot_index = jnp.argmax(replica_table == expert).astype(jnp.int32)
            gate_mat = lax.dynamic_index_in_dim(w_gate, slot_index, 0, keepdims=False)
            up_mat = lax.dynamic_index_in_dim(w_up, slot_index, 0, keepdims=False)
            down_mat = lax.dynamic_index_in_dim(w_down, slot_index, 0, keepdims=False)
            is_named = pick_ids == expert
            weight = jnp.sum(jnp.where(is_named, gate_vals, 0.0), axis=1)
            has_expert = jnp.any(is_named, axis=1)
            row_index = jnp.nonzero(has_expert, size=most_rows, fill_value=row_total)[0].astype(jnp.int32)
            chosen = jnp.take(section_rows, row_index, axis=0, mode="clip")
            gate_proj = jnp.dot(chosen, gate_mat, preferred_element_type=jnp.float32)
            up_proj = jnp.dot(chosen, up_mat, preferred_element_type=jnp.float32)
            hidden = (jax.nn.silu(gate_proj) * up_proj).astype(jnp.bfloat16)
            blocks = hidden.reshape(most_rows, N_LOCAL, HID_DEV).astype(jnp.float32)
            down_blocks = down_mat.reshape(N_LOCAL, HID_DEV, D).astype(jnp.float32)
            block_pieces = jnp.einsum("rbh,bhd->rbd", blocks, down_blocks, precision=lax.Precision.HIGHEST).astype(jnp.bfloat16)
            expert_out = jnp.sum(block_pieces.astype(jnp.float32), axis=1).astype(jnp.bfloat16)
            pick_scale = jnp.take(weight, row_index, mode="clip")
            accum_out = accum_out.at[row_index].add(pick_scale[:, None] * expert_out.astype(jnp.float32), mode="drop")
        return accum_out.astype(jnp.bfloat16)

    layer_out = lax.map(one_section, (tokens, routes, route_gates))
    return jnp.concatenate([jnp.zeros_like(layer_out[:1]), layer_out[:-1]], axis=0)
```

```python
import functools

import jax
import jax.numpy as jnp
from jax import lax
from jax.experimental import pallas as pl
from jax.experimental.pallas import tpu as pltpu
from jax.sharding import PartitionSpec as P

CAP = 2
G = 8
B = CAP * G
KEEP = 24 * 1024 * 1024
SPLIT = 4
MESH = pl.DeviceIdType.MESH


def row_piece(shape):
    return lax.broadcasted_iota(jnp.int32, shape, 0) % G


def relay_kernel(
    n_section, n_node, n_local,
    table_hbm, routes_hbm, gates_hbm, tok_hbm, wg_hbm, wu_hbm, wd_hbm,
    rows_ref, mix_ref,
    table_ref, routes_ref, gates_ref, ids, vals, tok, wg, wu, wd, disp, recv, outb, ret, comb_own, comb_in,
    in_sem, tok_sem, w_sem, send_sem, recv_sem, back_sem, ret_sem, comb_send, comb_recv,
):
    s = lax.axis_index("section")
    n = lax.axis_index("node")
    l = lax.axis_index("local")
    odd = n % 2
    sources = n_node * n_local
    me = n * n_local + l
    tok_dev, width = tok_hbm.shape
    piece = width // G
    tok_pad = ids.shape[1]
    hid = wg_hbm.shape[1]
    sends = s < n_section - 1
    owns = s > 0
    works = jnp.logical_and(s + odd > 0, s + odd < n_section)

    others = sorted(
        ((dn, dl) for dn in range(n_node) for dl in range(n_local) if dn or dl),
        key=lambda d: (d[0] == 0) + (d[1] == 0) + (d[0] % 2) / 4,
    )

    def cols(k):
        return pl.ds(k * piece, piece)

    tok_copies = [
        pltpu.make_async_copy(
            tok_hbm.at[:, cols(k)], tok.at[pl.ds(k * tok_pad, tok_dev)], tok_sem.at[k]
        )
        for k in range(G)
    ]
    w_copies = [
        pltpu.make_async_copy(
            hbm.at[pl.ds(i * hbm.shape[0] // SPLIT, hbm.shape[0] // SPLIT)],
            held.at[pl.ds(i * hbm.shape[0] // SPLIT, hbm.shape[0] // SPLIT)],
            w_sem.at[w * SPLIT + i],
        )
        for w, (hbm, held) in enumerate(((wg_hbm, wg), (wu_hbm, wu), (wd_hbm, wd)))
        for i in range(SPLIT)
    ]
    in_copies = [
        pltpu.make_async_copy(table_hbm, table_ref, in_sem.at[0]),
        pltpu.make_async_copy(routes_hbm, routes_ref, in_sem.at[1]),
        pltpu.make_async_copy(gates_hbm, gates_ref, in_sem.at[2]),
    ]

    barrier = pltpu.get_barrier_semaphore()

    def greet(section, places):
        for dn, dl in places:
            pl.semaphore_signal(
                barrier, inc=1,
                device_id=(section, (n + dn) % n_node, (l + dl) % n_local),
                device_id_type=MESH,
            )

    @pl.when(owns)
    def _():
        greet(s - 1, others + [(0, 0)])

    greet(s, others)
    for c in in_copies + tok_copies:
        c.start()
    for c in in_copies:
        c.wait()

    ids[...] = jnp.full(ids.shape, -1, jnp.int32)
    vals[...] = jnp.zeros(vals.shape, jnp.float32)
    ids[:, :tok_dev] = routes_ref[...]
    vals[:, :tok_dev] = gates_ref[...]
    picks = ids[...]
    gates = vals[...]
    named_rows = max(16, n_node)
    row_id = lax.broadcasted_iota(jnp.int32, (named_rows, tok_pad), 0)
    named = jnp.zeros((named_rows, tok_pad), jnp.float32)
    hits, weights = [], []
    for j in range(n_node):
        hit = picks == table_ref[j]
        hits.append(jnp.max(jnp.where(hit, 1.0, 0.0), axis=0, keepdims=True))
        weights.append(jnp.sum(jnp.where(hit, gates, 0.0), axis=0, keepdims=True))
        named = jnp.where(row_id == j, hits[j], named)
    before = lax.broadcasted_iota(jnp.int32, (tok_pad, tok_pad), 0) < lax.broadcasted_iota(
        jnp.int32, (tok_pad, tok_pad), 1
    )
    rank = jnp.dot(
        named.astype(jnp.bfloat16),
        jnp.where(before, 1.0, 0.0).astype(jnp.bfloat16),
        preferred_element_type=jnp.float32,
    ).astype(jnp.int32)
    chosen = []
    for j in range(n_node):
        copies = jnp.int32(0)
        replica = jnp.int32(0)
        for i in range(n_node):
            same = (table_ref[i] == table_ref[j]).astype(jnp.int32)
            copies = copies + same
            if i < j:
                replica = replica + same
        for p in range(CAP):
            want = p * copies + replica
            sel = jnp.where(rank[j : j + 1] == want, hits[j], 0.0)
            comb_own[j * CAP + p : j * CAP + p + 1, :] = sel * weights[j]
            chosen.append(jnp.broadcast_to(sel, (G, tok_pad)))
    chosen = jnp.concatenate(chosen, axis=0)
    piece_of = row_piece(chosen.shape)
    select = jnp.concatenate(
        [jnp.where(piece_of == k, chosen, 0.0).astype(jnp.bfloat16) for k in range(G)], axis=1
    )
    if tok_pad > tok_dev:
        for k in range(G):
            tok[k * tok_pad + tok_dev : (k + 1) * tok_pad, :] = jnp.zeros(
                (tok_pad - tok_dev, piece), jnp.bfloat16
            )
    for c in tok_copies:
        c.wait()
    for c in w_copies:
        c.start()
    disp[...] = jnp.dot(select, tok[...], preferred_element_type=jnp.float32).astype(jnp.bfloat16)

    around = (sources - 1) + sources * sends.astype(jnp.int32)
    pl.semaphore_wait(barrier, around)

    def dispatch(dn, dl):
        j = (n + dn) % n_node
        m = (l + dl) % n_local
        return pltpu.make_async_remote_copy(
            src_ref=disp.at[pl.ds(pl.multiple_of(j * B, B), B)],
            dst_ref=recv.at[pl.ds(pl.multiple_of(me * B, B), B)],
            send_sem=send_sem.at[dn * n_local + dl],
            recv_sem=recv_sem.at[me],
            device_id=(s + 1 - j % 2, j, m),
            device_id_type=MESH,
        )

    own_in = pltpu.make_async_copy(
        disp.at[pl.ds(pl.multiple_of(n * B, B), B)],
        recv.at[pl.ds(pl.multiple_of(me * B, B), B)],
        recv_sem.at[me],
    )
    comb_copy = pltpu.make_async_remote_copy(
        src_ref=comb_own, dst_ref=comb_in, send_sem=comb_send.at[0], recv_sem=comb_recv.at[0],
        device_id=(s + 1, n, l), device_id_type=MESH,
    )
    @pl.when(sends)
    def _():
        for dn, dl in others:
            dispatch(dn, dl).start()

        @pl.when(odd == 0)
        def _():
            dispatch(0, 0).start()

        @pl.when(odd == 1)
        def _():
            own_in.start()

        comb_copy.start()

    def give_back(dn, dl):
        qn = (n + dn) % n_node
        ql = (l + dl) % n_local
        q = qn * n_local + ql
        return pltpu.make_async_remote_copy(
            src_ref=outb.at[pl.ds(pl.multiple_of(q * B, B), B)],
            dst_ref=ret.at[l, pl.ds(pl.multiple_of(n * B, B), B)],
            send_sem=back_sem.at[dn * n_local + dl],
            recv_sem=ret_sem.at[me],
            device_id=(s + odd, qn, ql),
            device_id_type=MESH,
        )

    own_back = pltpu.make_async_copy(
        outb.at[pl.ds(pl.multiple_of(me * B, B), B)],
        ret.at[l, pl.ds(pl.multiple_of(n * B, B), B)],
        ret_sem.at[me],
    )

    for c in w_copies:
        c.wait()

    @pl.when(works)
    def _():
        for q in range(sources):
            block = recv.at[pl.ds(q * B, B)]
            pltpu.make_async_copy(block, block, recv_sem.at[q]).wait()
        rows = recv[...]
        piece_id = row_piece((sources * B, 2 * hid))
        total = jnp.zeros((sources * B, 2 * hid), jnp.float32)
        for k in range(G):
            both = jnp.concatenate(
                [wg[k * piece : (k + 1) * piece, :], wu[k * piece : (k + 1) * piece, :]], axis=1
            )
            part = jnp.dot(rows, both, preferred_element_type=jnp.float32)
            total = total + jnp.where(piece_id == k, part, 0.0)
        total = total.reshape(sources * CAP, G, 2 * hid)
        total = jnp.broadcast_to(jnp.sum(total, axis=1, keepdims=True), total.shape)
        total = total.reshape(sources * B, 2 * hid)
        gate_proj = total[:, :hid]
        up_proj = total[:, hid:]
        hidden = gate_proj / (1.0 + jnp.exp(-gate_proj)) * up_proj
        piece_h = row_piece(hidden.shape)
        spread = jnp.concatenate(
            [jnp.where(piece_h == k, hidden, 0.0).astype(jnp.bfloat16) for k in range(G)], axis=1
        )
        down = jnp.concatenate([wd[:, k * piece : (k + 1) * piece] for k in range(G)], axis=0)
        outb[...] = jnp.dot(spread, down, preferred_element_type=jnp.float32).astype(
            jnp.bfloat16
        )
        for dn, dl in others:
            give_back(dn, dl).start()

        @pl.when(odd == 1)
        def _():
            give_back(0, 0).start()

        @pl.when(odd == 0)
        def _():
            own_back.start()

    @pl.when(owns)
    def _():
        comb_copy.wait_recv()
        mix = comb_in[...]
        high = mix.astype(jnp.bfloat16).astype(jnp.float32)
        tall = jnp.concatenate(
            [
                jnp.broadcast_to(part[c : c + 1], (G, tok_pad))
                for part in (high, mix - high)
                for c in range(n_node * CAP)
            ],
            axis=0,
        )
        mix_ref[...] = jnp.transpose(tall).astype(jnp.bfloat16)
        for q in range(sources):
            block = ret.at[q % n_local, pl.ds((q // n_local) * B, B)]
            pltpu.make_async_copy(block, block, ret_sem.at[q]).wait()
        summed = ret[0].astype(jnp.float32)
        for m in range(1, n_local):
            summed = summed + ret[m].astype(jnp.float32)
        rows_ref[...] = summed.astype(jnp.bfloat16)

    @pl.when(s == 0)
    def _():
        rows_ref[...] = jnp.zeros(rows_ref.shape, jnp.bfloat16)
        mix_ref[...] = jnp.zeros(mix_ref.shape, jnp.bfloat16)

    @pl.when(sends)
    def _():
        for dn, dl in others:
            dispatch(dn, dl).wait_send()

        @pl.when(odd == 0)
        def _():
            dispatch(0, 0).wait_send()

        comb_copy.wait_send()

    @pl.when(works)
    def _():
        for dn, dl in others:
            give_back(dn, dl).wait_send()

        @pl.when(odd == 1)
        def _():
            give_back(0, 0).wait_send()


def expand_kernel(rows_ref, mix_ref, out_hbm, obuf, sem):
    tok_dev = out_hbm.shape[0]
    piece = rows_ref.shape[1]
    rows = rows_ref[...]
    rows = jnp.concatenate([rows, rows], axis=0)
    mix = mix_ref[:tok_dev, :].astype(jnp.float32)
    lane = lax.broadcasted_iota(jnp.int32, mix.shape, 1) % G
    copies = []
    for k in range(G):
        left = jnp.where(lane == k, mix, 0.0).astype(jnp.bfloat16)
        obuf[k] = jnp.dot(left, rows, preferred_element_type=jnp.float32).astype(jnp.bfloat16)
        copy = pltpu.make_async_copy(
            obuf.at[k], out_hbm.at[:, pl.ds(k * piece, piece)], sem.at[k]
        )
        copy.start()
        copies.append(copy)
    for copy in copies:
        copy.wait()


def shards(n_section, tokens, routes, route_gates, replica_table, w_gate, w_up, w_down):
    n_node = lax.axis_size("node")
    n_local = lax.axis_size("local")
    sources = n_node * n_local
    tok_dev, width = tokens.shape[1:]
    topk = routes.shape[2]
    hid = w_gate.shape[2]
    piece = width // G
    tok_pad = -(-tok_dev // 128) * 128
    slots = n_node * CAP
    vmem = pl.BlockSpec(memory_space=pltpu.VMEM)
    hbm = pl.BlockSpec(memory_space=pltpu.HBM)
    rows, mix = pl.pallas_call(
        functools.partial(relay_kernel, n_section, n_node, n_local),
        out_shape=(
            pltpu.VMEM((n_node * B, piece), jnp.bfloat16),
            pltpu.VMEM((tok_pad, 2 * slots * G), jnp.bfloat16),
        ),
        in_specs=[hbm] * 7,
        out_specs=(vmem, vmem),
        scratch_shapes=[
            pltpu.SMEM((n_node,), jnp.int32),
            pltpu.VMEM((topk, tok_dev), jnp.int32),
            pltpu.VMEM((topk, tok_dev), jnp.float32),
            pltpu.VMEM((topk, tok_pad), jnp.int32),
            pltpu.VMEM((topk, tok_pad), jnp.float32),
            pltpu.VMEM((G * tok_pad, piece), jnp.bfloat16),
            pltpu.VMEM((width, hid), jnp.bfloat16),
            pltpu.VMEM((width, hid), jnp.bfloat16),
            pltpu.VMEM((hid, width), jnp.bfloat16),
            pltpu.VMEM((n_node * B, piece), jnp.bfloat16),
            pltpu.VMEM((sources * B, piece), jnp.bfloat16),
            pltpu.VMEM((sources * B, piece), jnp.bfloat16),
            pltpu.VMEM((n_local, n_node * B, piece), jnp.bfloat16),
            pltpu.VMEM((slots, tok_pad), jnp.float32),
            pltpu.VMEM((slots, tok_pad), jnp.float32),
            pltpu.SemaphoreType.DMA((3,)),
            pltpu.SemaphoreType.DMA((G,)),
            pltpu.SemaphoreType.DMA((3 * SPLIT,)),
            pltpu.SemaphoreType.DMA((sources,)),
            pltpu.SemaphoreType.DMA((sources,)),
            pltpu.SemaphoreType.DMA((sources,)),
            pltpu.SemaphoreType.DMA((sources,)),
            pltpu.SemaphoreType.DMA((1,)),
            pltpu.SemaphoreType.DMA((1,)),
        ],
        compiler_params=pltpu.CompilerParams(
            collective_id=0, has_side_effects=True, vmem_limit_bytes=KEEP
        ),
        name="relay",
    )(
        *(
            pltpu.with_memory_space_constraint(a, pltpu.HBM)
            for a in (
                replica_table,
                jnp.transpose(routes[0]),
                jnp.transpose(route_gates[0]),
                tokens[0],
                w_gate[0],
                w_up[0],
                w_down[0],
            )
        )
    )
    out = pl.pallas_call(
        expand_kernel,
        out_shape=jax.ShapeDtypeStruct((tok_dev, width), jnp.bfloat16),
        in_specs=[vmem, vmem],
        out_specs=hbm,
        scratch_shapes=[
            pltpu.VMEM((G, tok_dev, piece), jnp.bfloat16),
            pltpu.SemaphoreType.DMA((G,)),
        ],
        compiler_params=pltpu.CompilerParams(vmem_limit_bytes=KEEP),
        name="expand",
    )(rows, mix)
    return out[None]


def solution(mesh):
    placed = (
        P("section", ("node", "local"), None),
        P("section", ("node", "local"), None),
        P("section", ("node", "local"), None),
        P(),
        P("node", None, "local"),
        P("node", None, "local"),
        P("node", "local", None),
    )
    return jax.shard_map(
        functools.partial(shards, mesh.shape["section"]),
        mesh=mesh,
        in_specs=placed,
        out_specs=P("section", ("node", "local"), None),
        check_vma=False,
    )
```

```python
import functools

import jax
import jax.numpy as jnp
from jax import lax
from jax.experimental import pallas as pl
from jax.experimental.pallas import tpu as pltpu
from jax.sharding import PartitionSpec as P

CAP = 2
G = 8
B = CAP * G
KEEP = 24 * 1024 * 1024
SPLIT = 4
MESH = pl.DeviceIdType.MESH


def row_piece(shape):
    return lax.broadcasted_iota(jnp.int32, shape, 0) % G


def relay_kernel(
    n_section, n_node, n_local,
    table_hbm, routes_hbm, gates_hbm, tok_hbm, wg_hbm, wu_hbm, wd_hbm,
    rows_ref, mix_ref,
    table_ref, routes_ref, gates_ref, ids, vals, tok, wg, wu, wd, disp, recv, outb, ret, comb_own, comb_in,
    in_sem, tok_sem, w_sem, send_sem, recv_sem, back_sem, ret_sem, comb_send, comb_recv, up_sem,
):
    s = lax.axis_index("section")
    n = lax.axis_index("node")
    l = lax.axis_index("local")
    core = n % 2
    chips = n_node // 2
    sources = n_node * n_local
    tok_dev, width = tok_hbm.shape
    piece = width // G
    tok_pad = ids.shape[1]
    hid = wg_hbm.shape[1]
    sends = s < n_section - 1
    owns = s > 0

    home = (0, 0)
    moves = sorted(
        ((dx, dl) for dx in range(chips) for dl in range(n_local)),
        key=lambda d: -min(d[0], chips - d[0]) - min(d[1], n_local - d[1]),
    )
    here = [d for d in moves if (d[0] + d[1]) % 2 == 0]
    above = [d for d in moves if (d[0] + d[1]) % 2 == 1]
    slots = here + above
    near_rows = len(here) * 2 * B

    def place(move, side):
        return (n // 2 + move[0]) % chips * 2 + side, (l + move[1]) % n_local

    def back(move):
        return -move[0], -move[1]

    def cols(k):
        return pl.ds(k * piece, piece)

    tok_copies = [
        pltpu.make_async_copy(
            tok_hbm.at[:, cols(k)], tok.at[pl.ds(k * tok_pad, tok_dev)], tok_sem.at[k]
        )
        for k in range(G)
    ]
    w_copies = [
        pltpu.make_async_copy(
            hbm.at[pl.ds(i * hbm.shape[0] // SPLIT, hbm.shape[0] // SPLIT)],
            held.at[pl.ds(i * hbm.shape[0] // SPLIT, hbm.shape[0] // SPLIT)],
            w_sem.at[w * SPLIT + i],
        )
        for w, (hbm, held) in enumerate(((wg_hbm, wg), (wu_hbm, wu), (wd_hbm, wd)))
        for i in range(SPLIT)
    ]
    in_copies = [
        pltpu.make_async_copy(table_hbm, table_ref, in_sem.at[0]),
        pltpu.make_async_copy(routes_hbm, routes_ref, in_sem.at[1]),
        pltpu.make_async_copy(gates_hbm, gates_ref, in_sem.at[2]),
    ]

    barrier = pltpu.get_barrier_semaphore()

    def greet(section, move, side):
        j, m = place(move, side)
        pl.semaphore_signal(barrier, inc=1, device_id=(section, j, m), device_id_type=MESH)

    for move in moves:
        for flip in range(2):
            if move != home or flip:
                greet(s, move, core ^ flip)

    callers = [(back(move), flip) for move in above for flip in range(2)] + [(home, 0)]

    @pl.when(owns)
    def _():
        for move, flip in callers:
            greet(s - 1, move, core ^ flip)

    @pl.when(sends)
    def _():
        greet(s + 1, home, core)

    for c in in_copies + tok_copies:
        c.start()
    for c in in_copies:
        c.wait()

    ids[...] = jnp.full(ids.shape, -1, jnp.int32)
    vals[...] = jnp.zeros(vals.shape, jnp.float32)
    ids[:, :tok_dev] = routes_ref[...]
    vals[:, :tok_dev] = gates_ref[...]
    picks = ids[...]
    gates = vals[...]
    named_rows = max(16, n_node)
    row_id = lax.broadcasted_iota(jnp.int32, (named_rows, tok_pad), 0)
    named = jnp.zeros((named_rows, tok_pad), jnp.float32)
    hits, weights = [], []
    for j in range(n_node):
        hit = picks == table_ref[j]
        hits.append(jnp.max(jnp.where(hit, 1.0, 0.0), axis=0, keepdims=True))
        weights.append(jnp.sum(jnp.where(hit, gates, 0.0), axis=0, keepdims=True))
        named = jnp.where(row_id == j, hits[j], named)
    before = lax.broadcasted_iota(jnp.int32, (tok_pad, tok_pad), 0) < lax.broadcasted_iota(
        jnp.int32, (tok_pad, tok_pad), 1
    )
    rank = jnp.dot(
        named.astype(jnp.bfloat16),
        jnp.where(before, 1.0, 0.0).astype(jnp.bfloat16),
        preferred_element_type=jnp.float32,
    ).astype(jnp.int32)
    chosen = []
    for j in range(n_node):
        copies = jnp.int32(0)
        replica = jnp.int32(0)
        for i in range(n_node):
            same = (table_ref[i] == table_ref[j]).astype(jnp.int32)
            copies = copies + same
            if i < j:
                replica = replica + same
        for p in range(CAP):
            want = p * copies + replica
            sel = jnp.where(rank[j : j + 1] == want, hits[j], 0.0)
            comb_own[j * CAP + p : j * CAP + p + 1, :] = sel * weights[j]
            chosen.append(jnp.broadcast_to(sel, (G, tok_pad)))
    chosen = jnp.concatenate(chosen, axis=0)
    piece_of = row_piece(chosen.shape)
    select = jnp.concatenate(
        [jnp.where(piece_of == k, chosen, 0.0).astype(jnp.bfloat16) for k in range(G)], axis=1
    )
    if tok_pad > tok_dev:
        for k in range(G):
            tok[k * tok_pad + tok_dev : (k + 1) * tok_pad, :] = jnp.zeros(
                (tok_pad - tok_dev, piece), jnp.bfloat16
            )
    for c in tok_copies:
        c.wait()
    for c in w_copies:
        c.start()
    def dispatch(move, side, up):
        j, m = place(move, side)
        return pltpu.make_async_remote_copy(
            src_ref=disp.at[pl.ds(pl.multiple_of(j * B, B), B)],
            dst_ref=recv.at[block_of(move, core)],
            send_sem=send_sem.at[0],
            recv_sem=recv_sem.at[up],
            device_id=(s + up, j, m),
            device_id_type=MESH,
        )

    def block_of(move, side):
        return pl.ds(pl.multiple_of((slots.index(move) * 2 + side) * B, B), B)

    def own_in():
        return pltpu.make_async_copy(
            disp.at[pl.ds(pl.multiple_of(n * B, B), B)],
            recv.at[block_of(home, core)],
            recv_sem.at[0],
        )

    comb_copy = pltpu.make_async_remote_copy(
        src_ref=comb_own, dst_ref=comb_in, send_sem=comb_send.at[0], recv_sem=comb_recv.at[0],
        device_id=(s + 1, n, l), device_id_type=MESH,
    )
    disp[...] = jnp.dot(select, tok[...], preferred_element_type=jnp.float32).astype(
        jnp.bfloat16
    )
    pl.semaphore_wait(
        barrier,
        sources - 1 + len(callers) * sends.astype(jnp.int32) + owns.astype(jnp.int32),
    )

    @pl.when(owns)
    def _():
        pl.semaphore_signal(up_sem, inc=1, device_id=(s - 1, n, l), device_id_type=MESH)

    @pl.when(sends)
    def _():
        comb_copy.start()
        for move in here:
            for side in range(2):
                if move != home:
                    dispatch(move, side, 0).start()
        for move in above:
            for side in range(2):
                dispatch(move, side, 1).start()
        dispatch(home, 1 - core, 0).start()
        own_in().start()

    def give_back(move, side, up):
        qn, ql = place(back(move), side)
        return pltpu.make_async_remote_copy(
            src_ref=outb.at[block_of(move, side)],
            dst_ref=ret.at[l, pl.ds(pl.multiple_of(n * B, B), B)],
            send_sem=back_sem.at[1 - up],
            recv_sem=ret_sem.at[0],
            device_id=(s + up, qn, ql),
            device_id_type=MESH,
        )

    for c in w_copies:
        c.wait()

    def drain(held, sem):
        pltpu.make_async_copy(held, held, sem).wait()

    @pl.when(sends)
    def _():
        drain(recv.at[:near_rows], recv_sem.at[0])

    @pl.when(owns)
    def _():
        drain(recv.at[near_rows:], recv_sem.at[1])

    rows = recv[...]
    piece_id = row_piece((sources * B, 2 * hid))
    total = jnp.zeros((sources * B, 2 * hid), jnp.float32)
    for k in range(G):
        span = slice(k * piece, (k + 1) * piece)
        both = jnp.concatenate([wg[span, :], wu[span, :]], axis=1)
        part = jnp.dot(rows, both, preferred_element_type=jnp.float32)
        total = total + jnp.where(piece_id == k, part, 0.0)
    total = total.reshape(sources * CAP, G, 2 * hid)
    total = jnp.broadcast_to(jnp.sum(total, axis=1, keepdims=True), total.shape)
    total = total.reshape(sources * B, 2 * hid)
    gate_proj = total[:, :hid]
    up_proj = total[:, hid:]
    hidden = gate_proj / (1.0 + jnp.exp(-gate_proj)) * up_proj
    piece_h = row_piece(hidden.shape)
    spread = jnp.concatenate(
        [jnp.where(piece_h == k, hidden, 0.0).astype(jnp.bfloat16) for k in range(G)], axis=1
    )

    down = jnp.concatenate([wd[:, k * piece : (k + 1) * piece] for k in range(G)], axis=0)
    outb[...] = jnp.dot(spread, down, preferred_element_type=jnp.float32).astype(jnp.bfloat16)

    @pl.when(sends)
    def _():
        pl.semaphore_wait(up_sem, 1)
        for move in here:
            for side in range(2):
                give_back(move, side, 1).start()

    @pl.when(owns)
    def _():
        for move in above:
            for side in range(2):
                give_back(move, side, 0).start()

    @pl.when(owns)
    def _():
        comb_copy.wait_recv()
        mix = comb_in[...]
        high = mix.astype(jnp.bfloat16).astype(jnp.float32)
        tall = jnp.concatenate(
            [
                jnp.broadcast_to(part[c : c + 1], (G, tok_pad))
                for part in (high, mix - high)
                for c in range(n_node * CAP)
            ],
            axis=0,
        )
        mix_ref[...] = jnp.transpose(tall).astype(jnp.bfloat16)
        drain(ret, ret_sem.at[0])
        summed = ret[0].astype(jnp.float32)
        for m in range(1, n_local):
            summed = summed + ret[m].astype(jnp.float32)
        rows_ref[...] = summed.astype(jnp.bfloat16)

    @pl.when(s == 0)
    def _():
        rows_ref[...] = jnp.zeros(rows_ref.shape, jnp.bfloat16)
        mix_ref[...] = jnp.zeros(mix_ref.shape, jnp.bfloat16)

    @pl.when(sends)
    def _():
        drain(recv.at[B:], send_sem.at[0])
        drain(outb.at[:near_rows], back_sem.at[0])
        comb_copy.wait_send()

    @pl.when(owns)
    def _():
        drain(outb.at[near_rows:], back_sem.at[1])


def expand_kernel(rows_ref, mix_ref, out_hbm, obuf, sem):
    tok_dev = out_hbm.shape[0]
    piece = rows_ref.shape[1]
    rows = rows_ref[...]
    rows = jnp.concatenate([rows, rows], axis=0)
    mix = mix_ref[:tok_dev, :].astype(jnp.float32)
    lane = lax.broadcasted_iota(jnp.int32, mix.shape, 1) % G
    copies = []
    for k in range(G):
        left = jnp.where(lane == k, mix, 0.0).astype(jnp.bfloat16)
        obuf[k] = jnp.dot(left, rows, preferred_element_type=jnp.float32).astype(jnp.bfloat16)
        copy = pltpu.make_async_copy(
            obuf.at[k], out_hbm.at[:, pl.ds(k * piece, piece)], sem.at[k]
        )
        copy.start()
        copies.append(copy)
    for copy in copies:
        copy.wait()


def shards(n_section, tokens, routes, route_gates, replica_table, w_gate, w_up, w_down):
    n_node = lax.axis_size("node")
    n_local = lax.axis_size("local")
    sources = n_node * n_local
    tok_dev, width = tokens.shape[1:]
    topk = routes.shape[2]
    hid = w_gate.shape[2]
    piece = width // G
    tok_pad = -(-tok_dev // 128) * 128
    slots = n_node * CAP
    vmem = pl.BlockSpec(memory_space=pltpu.VMEM)
    hbm = pl.BlockSpec(memory_space=pltpu.HBM)
    rows, mix = pl.pallas_call(
        functools.partial(relay_kernel, n_section, n_node, n_local),
        out_shape=(
            pltpu.VMEM((n_node * B, piece), jnp.bfloat16),
            pltpu.VMEM((tok_pad, 2 * slots * G), jnp.bfloat16),
        ),
        in_specs=[hbm] * 7,
        out_specs=(vmem, vmem),
        scratch_shapes=[
            pltpu.SMEM((n_node,), jnp.int32),
            pltpu.VMEM((topk, tok_dev), jnp.int32),
            pltpu.VMEM((topk, tok_dev), jnp.float32),
            pltpu.VMEM((topk, tok_pad), jnp.int32),
            pltpu.VMEM((topk, tok_pad), jnp.float32),
            pltpu.VMEM((G * tok_pad, piece), jnp.bfloat16),
            pltpu.VMEM((width, hid), jnp.bfloat16),
            pltpu.VMEM((width, hid), jnp.bfloat16),
            pltpu.VMEM((hid, width), jnp.bfloat16),
            pltpu.VMEM((n_node * B, piece), jnp.bfloat16),
            pltpu.VMEM((sources * B, piece), jnp.bfloat16),
            pltpu.VMEM((sources * B, piece), jnp.bfloat16),
            pltpu.VMEM((n_local, n_node * B, piece), jnp.bfloat16),
            pltpu.VMEM((slots, tok_pad), jnp.float32),
            pltpu.VMEM((slots, tok_pad), jnp.float32),
            pltpu.SemaphoreType.DMA((3,)),
            pltpu.SemaphoreType.DMA((G,)),
            pltpu.SemaphoreType.DMA((3 * SPLIT,)),
            pltpu.SemaphoreType.DMA((1,)),
            pltpu.SemaphoreType.DMA((2,)),
            pltpu.SemaphoreType.DMA((2,)),
            pltpu.SemaphoreType.DMA((1,)),
            pltpu.SemaphoreType.DMA((1,)),
            pltpu.SemaphoreType.DMA((1,)),
            pltpu.SemaphoreType.REGULAR,
        ],
        compiler_params=pltpu.CompilerParams(
            collective_id=0, has_side_effects=True, vmem_limit_bytes=KEEP
        ),
        name="relay",
    )(
        *(
            pltpu.with_memory_space_constraint(a, pltpu.HBM)
            for a in (
                replica_table,
                jnp.transpose(routes[0]),
                jnp.transpose(route_gates[0]),
                tokens[0],
                w_gate[0],
                w_up[0],
                w_down[0],
            )
        )
    )
    out = pl.pallas_call(
        expand_kernel,
        out_shape=jax.ShapeDtypeStruct((tok_dev, width), jnp.bfloat16),
        in_specs=[vmem, vmem],
        out_specs=hbm,
        scratch_shapes=[
            pltpu.VMEM((G, tok_dev, piece), jnp.bfloat16),
            pltpu.SemaphoreType.DMA((G,)),
        ],
        compiler_params=pltpu.CompilerParams(vmem_limit_bytes=KEEP),
        name="expand",
    )(rows, mix)
    return out[None]


def solution(mesh):
    placed = (
        P("section", ("node", "local"), None),
        P("section", ("node", "local"), None),
        P("section", ("node", "local"), None),
        P(),
        P("node", None, "local"),
        P("node", None, "local"),
        P("node", "local", None),
    )
    return jax.shard_map(
        functools.partial(shards, mesh.shape["section"]),
        mesh=mesh,
        in_specs=placed,
        out_specs=P("section", ("node", "local"), None),
        check_vma=False,
    )
```

```python
import functools

import jax
import jax.numpy as jnp
from jax import lax
from jax.experimental import pallas as pl
from jax.experimental.pallas import tpu as pltpu
from jax.sharding import PartitionSpec as P

CAP = 2
G = 8
B = CAP * G
KEEP = 24 * 1024 * 1024
SPLIT = 4
MESH = pl.DeviceIdType.MESH


def row_piece(shape):
    return lax.broadcasted_iota(jnp.int32, shape, 0) % G


def relay_kernel(
    n_section, n_node, n_local,
    table_hbm, routes_hbm, gates_hbm, tok_hbm, wg_hbm, wu_hbm, wd_hbm,
    rows_ref, mix_ref,
    table_ref, routes_ref, gates_ref, ids, vals, tok, wg, wu, wd, disp, recv, outb, ret, comb_own, comb_in,
    in_sem, tok_sem, w_sem, send_sem, recv_sem, back_sem, ret_sem, comb_send, comb_recv, up_sem,
):
    s = lax.axis_index("section")
    n = lax.axis_index("node")
    l = lax.axis_index("local")
    core = n % 2
    chips = n_node // 2
    sources = n_node * n_local
    tok_dev, width = tok_hbm.shape
    piece = width // G
    tok_pad = ids.shape[1]
    hid = wg_hbm.shape[1]
    sends = s < n_section - 1
    owns = s > 0

    home = (0, 0)
    moves = sorted(
        ((dx, dl) for dx in range(chips) for dl in range(n_local)),
        key=lambda d: -min(d[0], chips - d[0]) - min(d[1], n_local - d[1]),
    )
    here = [d for d in moves if d[1] % 2 == 1]
    above = [d for d in moves if d not in here]
    waves = [[d for d in moves if (d[0] + d[1]) % 2 == odd] for odd in range(2)]
    waves = [[d for d in wave if d in here] + [d for d in wave if d in above] for wave in waves]
    slots = waves[0] + waves[1]

    def drain(held, sem):
        pltpu.make_async_copy(held, held, sem).wait()

    def span(group):
        low = slots.index(group[0]) * 2 * B
        return slice(low, low + len(group) * 2 * B)

    def place(move, side):
        return (n // 2 + move[0]) % chips * 2 + side, (l + move[1]) % n_local

    def back(move):
        return -move[0], -move[1]

    def cols(k):
        return pl.ds(k * piece, piece)

    tok_copies = [
        pltpu.make_async_copy(
            tok_hbm.at[:, cols(k)], tok.at[pl.ds(k * tok_pad, tok_dev)], tok_sem.at[k]
        )
        for k in range(G)
    ]
    w_copies = [
        pltpu.make_async_copy(
            hbm.at[pl.ds(i * hbm.shape[0] // SPLIT, hbm.shape[0] // SPLIT)],
            held.at[pl.ds(i * hbm.shape[0] // SPLIT, hbm.shape[0] // SPLIT)],
            w_sem.at[w * SPLIT + i],
        )
        for w, (hbm, held) in enumerate(((wg_hbm, wg), (wu_hbm, wu), (wd_hbm, wd)))
        for i in range(SPLIT)
    ]
    in_copies = [
        pltpu.make_async_copy(table_hbm, table_ref, in_sem.at[0]),
        pltpu.make_async_copy(routes_hbm, routes_ref, in_sem.at[1]),
        pltpu.make_async_copy(gates_hbm, gates_ref, in_sem.at[2]),
    ]

    barrier = pltpu.get_barrier_semaphore()

    def greet(section, move, side):
        j, m = place(move, side)
        pl.semaphore_signal(barrier, inc=1, device_id=(section, j, m), device_id_type=MESH)

    for move in moves:
        for flip in range(2):
            if move != home or flip:
                greet(s, move, core ^ flip)

    callers = [(home, flip) for flip in range(2)]

    @pl.when(owns)
    def _():
        for move, flip in callers:
            greet(s - 1, move, core ^ flip)

    @pl.when(sends)
    def _():
        greet(s + 1, home, core)

    for c in in_copies + tok_copies:
        c.start()
    for c in in_copies:
        c.wait()

    ids[...] = jnp.full(ids.shape, -1, jnp.int32)
    vals[...] = jnp.zeros(vals.shape, jnp.float32)
    ids[:, :tok_dev] = routes_ref[...]
    vals[:, :tok_dev] = gates_ref[...]
    picks = ids[...]
    gates = vals[...]
    named_rows = max(16, n_node)
    row_id = lax.broadcasted_iota(jnp.int32, (named_rows, tok_pad), 0)
    named = jnp.zeros((named_rows, tok_pad), jnp.float32)
    hits, weights = [], []
    for j in range(n_node):
        hit = picks == table_ref[j]
        hits.append(jnp.max(jnp.where(hit, 1.0, 0.0), axis=0, keepdims=True))
        weights.append(jnp.sum(jnp.where(hit, gates, 0.0), axis=0, keepdims=True))
        named = jnp.where(row_id == j, hits[j], named)
    before = lax.broadcasted_iota(jnp.int32, (tok_pad, tok_pad), 0) < lax.broadcasted_iota(
        jnp.int32, (tok_pad, tok_pad), 1
    )
    rank = jnp.dot(
        named.astype(jnp.bfloat16),
        jnp.where(before, 1.0, 0.0).astype(jnp.bfloat16),
        preferred_element_type=jnp.float32,
    ).astype(jnp.int32)
    chosen = []
    for j in range(n_node):
        copies = jnp.int32(0)
        replica = jnp.int32(0)
        for i in range(n_node):
            same = (table_ref[i] == table_ref[j]).astype(jnp.int32)
            copies = copies + same
            if i < j:
                replica = replica + same
        for p in range(CAP):
            want = p * copies + replica
            sel = jnp.where(rank[j : j + 1] == want, hits[j], 0.0)
            comb_own[j * CAP + p : j * CAP + p + 1, :] = sel * weights[j]
            chosen.append(jnp.broadcast_to(sel, (G, tok_pad)))
    chosen = jnp.concatenate(chosen, axis=0)
    piece_of = row_piece(chosen.shape)
    select = jnp.concatenate(
        [jnp.where(piece_of == k, chosen, 0.0).astype(jnp.bfloat16) for k in range(G)], axis=1
    )
    if tok_pad > tok_dev:
        for k in range(G):
            tok[k * tok_pad + tok_dev : (k + 1) * tok_pad, :] = jnp.zeros(
                (tok_pad - tok_dev, piece), jnp.bfloat16
            )
    for c in tok_copies:
        c.wait()
    for c in w_copies:
        c.start()
    def dispatch(move, side):
        j, m = place(move, side)
        wave = int(move in waves[1])
        up = int(move in above)
        return pltpu.make_async_remote_copy(
            src_ref=disp.at[pl.ds(pl.multiple_of(j * B, B), B)],
            dst_ref=recv.at[block_of(move, core)],
            send_sem=send_sem.at[wave],
            recv_sem=recv_sem.at[wave, up],
            device_id=(s + up, j, m),
            device_id_type=MESH,
        )

    def block_of(move, side):
        return pl.ds(pl.multiple_of((slots.index(move) * 2 + side) * B, B), B)

    comb_copy = pltpu.make_async_remote_copy(
        src_ref=comb_own, dst_ref=comb_in, send_sem=comb_send.at[0], recv_sem=comb_recv.at[0],
        device_id=(s + 1, n, l), device_id_type=MESH,
    )
    disp[...] = jnp.dot(select, tok[...], preferred_element_type=jnp.float32).astype(
        jnp.bfloat16
    )
    pl.semaphore_wait(
        barrier,
        sources - 1 + len(callers) * sends.astype(jnp.int32) + owns.astype(jnp.int32),
    )

    @pl.when(owns)
    def _():
        pl.semaphore_signal(up_sem, inc=1, device_id=(s - 1, n, l), device_id_type=MESH)

    @pl.when(sends)
    def _():
        for move in waves[0]:
            for side in range(2):
                dispatch(move, side).start()
        comb_copy.start()
        pl.semaphore_wait(up_sem, 1)
        for move in waves[1]:
            for side in range(2):
                dispatch(move, side).start()

    def give_back(move, side):
        qn, ql = place(back(move), side)
        up = int(move in here)
        return pltpu.make_async_remote_copy(
            src_ref=outb.at[block_of(move, side)],
            dst_ref=ret.at[l, pl.ds(pl.multiple_of(n * B, B), B)],
            send_sem=back_sem.at[up],
            recv_sem=ret_sem.at[0],
            device_id=(s + up, qn, ql),
            device_id_type=MESH,
        )

    for c in w_copies:
        c.wait()

    for number, wave in enumerate(waves):
        stay = [move for move in wave if move in here]
        rise = [move for move in wave if move in above]

        @pl.when(sends)
        def _():
            drain(recv.at[span(stay)], recv_sem.at[number, 0])

        @pl.when(owns)
        def _():
            drain(recv.at[span(rise)], recv_sem.at[number, 1])

        rows = recv[span(wave), :]
        count = rows.shape[0]
        piece_id = row_piece((count, 2 * hid))
        total = jnp.zeros((count, 2 * hid), jnp.float32)
        for k in range(G):
            cut = slice(k * piece, (k + 1) * piece)
            both = jnp.concatenate([wg[cut, :], wu[cut, :]], axis=1)
            part = jnp.dot(rows, both, preferred_element_type=jnp.float32)
            total = total + jnp.where(piece_id == k, part, 0.0)
        total = total.reshape(count // G, G, 2 * hid)
        total = jnp.broadcast_to(jnp.sum(total, axis=1, keepdims=True), total.shape)
        total = total.reshape(count, 2 * hid)
        gate_proj = total[:, :hid]
        up_proj = total[:, hid:]
        hidden = gate_proj / (1.0 + jnp.exp(-gate_proj)) * up_proj
        piece_h = row_piece(hidden.shape)
        spread = jnp.concatenate(
            [jnp.where(piece_h == k, hidden, 0.0).astype(jnp.bfloat16) for k in range(G)],
            axis=1,
        )
        down = jnp.concatenate([wd[:, k * piece : (k + 1) * piece] for k in range(G)], axis=0)
        outb[span(wave), :] = jnp.dot(
            spread, down, preferred_element_type=jnp.float32
        ).astype(jnp.bfloat16)

        @pl.when(sends)
        def _():
            for move in stay:
                for side in range(2):
                    give_back(move, side).start()

        @pl.when(owns)
        def _():
            for move in rise:
                if move != home:
                    for side in range(2):
                        give_back(move, side).start()
                else:
                    give_back(move, 1 - core).start()
                    pltpu.make_async_copy(
                        outb.at[block_of(home, core)],
                        ret.at[l, pl.ds(pl.multiple_of(n * B, B), B)],
                        ret_sem.at[0],
                    ).start()

    @pl.when(owns)
    def _():
        comb_copy.wait_recv()
        mix = comb_in[...]
        high = mix.astype(jnp.bfloat16).astype(jnp.float32)
        tall = jnp.concatenate(
            [
                jnp.broadcast_to(part[c : c + 1], (G, tok_pad))
                for part in (high, mix - high)
                for c in range(n_node * CAP)
            ],
            axis=0,
        )
        mix_ref[...] = jnp.transpose(tall).astype(jnp.bfloat16)
        drain(ret, ret_sem.at[0])
        summed = ret[0].astype(jnp.float32)
        for m in range(1, n_local):
            summed = summed + ret[m].astype(jnp.float32)
        rows_ref[...] = summed.astype(jnp.bfloat16)

    @pl.when(s == 0)
    def _():
        rows_ref[...] = jnp.zeros(rows_ref.shape, jnp.bfloat16)
        mix_ref[...] = jnp.zeros(mix_ref.shape, jnp.bfloat16)

    @pl.when(sends)
    def _():
        drain(recv.at[span(waves[0])], send_sem.at[0])
        drain(recv.at[span(waves[1])], send_sem.at[1])
        drain(outb.at[: len(here) * 2 * B], back_sem.at[1])
        comb_copy.wait_send()

    @pl.when(owns)
    def _():
        drain(outb.at[: len(above) * 2 * B - B], back_sem.at[0])


def expand_kernel(rows_ref, mix_ref, out_hbm, obuf, sem):
    tok_dev = out_hbm.shape[0]
    piece = rows_ref.shape[1]
    rows = rows_ref[...]
    rows = jnp.concatenate([rows, rows], axis=0)
    mix = mix_ref[:tok_dev, :].astype(jnp.float32)
    lane = lax.broadcasted_iota(jnp.int32, mix.shape, 1) % G
    copies = []
    for k in range(G):
        left = jnp.where(lane == k, mix, 0.0).astype(jnp.bfloat16)
        obuf[k] = jnp.dot(left, rows, preferred_element_type=jnp.float32).astype(jnp.bfloat16)
        copy = pltpu.make_async_copy(
            obuf.at[k], out_hbm.at[:, pl.ds(k * piece, piece)], sem.at[k]
        )
        copy.start()
        copies.append(copy)
    for copy in copies:
        copy.wait()


def shards(n_section, tokens, routes, route_gates, replica_table, w_gate, w_up, w_down):
    n_node = lax.axis_size("node")
    n_local = lax.axis_size("local")
    sources = n_node * n_local
    tok_dev, width = tokens.shape[1:]
    topk = routes.shape[2]
    hid = w_gate.shape[2]
    piece = width // G
    tok_pad = -(-tok_dev // 128) * 128
    slots = n_node * CAP
    vmem = pl.BlockSpec(memory_space=pltpu.VMEM)
    hbm = pl.BlockSpec(memory_space=pltpu.HBM)
    rows, mix = pl.pallas_call(
        functools.partial(relay_kernel, n_section, n_node, n_local),
        out_shape=(
            pltpu.VMEM((n_node * B, piece), jnp.bfloat16),
            pltpu.VMEM((tok_pad, 2 * slots * G), jnp.bfloat16),
        ),
        in_specs=[hbm] * 7,
        out_specs=(vmem, vmem),
        scratch_shapes=[
            pltpu.SMEM((n_node,), jnp.int32),
            pltpu.VMEM((topk, tok_dev), jnp.int32),
            pltpu.VMEM((topk, tok_dev), jnp.float32),
            pltpu.VMEM((topk, tok_pad), jnp.int32),
            pltpu.VMEM((topk, tok_pad), jnp.float32),
            pltpu.VMEM((G * tok_pad, piece), jnp.bfloat16),
            pltpu.VMEM((width, hid), jnp.bfloat16),
            pltpu.VMEM((width, hid), jnp.bfloat16),
            pltpu.VMEM((hid, width), jnp.bfloat16),
            pltpu.VMEM((n_node * B, piece), jnp.bfloat16),
            pltpu.VMEM((sources * B, piece), jnp.bfloat16),
            pltpu.VMEM((sources * B, piece), jnp.bfloat16),
            pltpu.VMEM((n_local, n_node * B, piece), jnp.bfloat16),
            pltpu.VMEM((slots, tok_pad), jnp.float32),
            pltpu.VMEM((slots, tok_pad), jnp.float32),
            pltpu.SemaphoreType.DMA((3,)),
            pltpu.SemaphoreType.DMA((G,)),
            pltpu.SemaphoreType.DMA((3 * SPLIT,)),
            pltpu.SemaphoreType.DMA((2,)),
            pltpu.SemaphoreType.DMA((2, 2)),
            pltpu.SemaphoreType.DMA((2,)),
            pltpu.SemaphoreType.DMA((1,)),
            pltpu.SemaphoreType.DMA((1,)),
            pltpu.SemaphoreType.DMA((1,)),
            pltpu.SemaphoreType.REGULAR,
        ],
        compiler_params=pltpu.CompilerParams(
            collective_id=0, has_side_effects=True, vmem_limit_bytes=KEEP
        ),
        name="relay",
    )(
        *(
            pltpu.with_memory_space_constraint(a, pltpu.HBM)
            for a in (
                replica_table,
                jnp.transpose(routes[0]),
                jnp.transpose(route_gates[0]),
                tokens[0],
                w_gate[0],
                w_up[0],
                w_down[0],
            )
        )
    )
    out = pl.pallas_call(
        expand_kernel,
        out_shape=jax.ShapeDtypeStruct((tok_dev, width), jnp.bfloat16),
        in_specs=[vmem, vmem],
        out_specs=hbm,
        scratch_shapes=[
            pltpu.VMEM((G, tok_dev, piece), jnp.bfloat16),
            pltpu.SemaphoreType.DMA((G,)),
        ],
        compiler_params=pltpu.CompilerParams(vmem_limit_bytes=KEEP),
        name="expand",
    )(rows, mix)
    return out[None]


def solution(mesh):
    placed = (
        P("section", ("node", "local"), None),
        P("section", ("node", "local"), None),
        P("section", ("node", "local"), None),
        P(),
        P("node", None, "local"),
        P("node", None, "local"),
        P("node", "local", None),
    )
    return jax.shard_map(
        functools.partial(shards, mesh.shape["section"]),
        mesh=mesh,
        in_specs=placed,
        out_specs=P("section", ("node", "local"), None),
        check_vma=False,
    )
```

```python
import functools

import jax
import jax.numpy as jnp
from jax import lax
from jax.experimental import pallas as pl
from jax.experimental.pallas import tpu as pltpu
from jax.sharding import PartitionSpec as P

CAP = 2
G = 8
B = CAP * G
KEEP = 24 * 1024 * 1024
SPLIT = 4
IN = 512
MESH = pl.DeviceIdType.MESH


def row_piece(shape):
    return lax.broadcasted_iota(jnp.int32, shape, 0) % G


def chunks(piece, step):
    return [(low, min(low + step, piece)) for low in range(0, piece, step)]


def relay_kernel(
    n_section, n_node, n_local,
    table_hbm, routes_hbm, gates_hbm, tok_hbm, wg_hbm, wu_hbm, wd_hbm,
    rows_ref, mix_ref,
    table_ref, routes_ref, gates_ref, ids, vals, tok, wg, wu, wd, disp, recv, outb, ret, comb_own, comb_in,
    in_sem, tok_sem, w_sem, send_sem, recv_sem, back_sem, ret_sem, comb_send, comb_recv, up_sem,
):
    s = lax.axis_index("section")
    n = lax.axis_index("node")
    l = lax.axis_index("local")
    core = n % 2
    chips = n_node // 2
    sources = n_node * n_local
    tok_dev, width = tok_hbm.shape
    piece = width // G
    tok_pad = ids.shape[1]
    hid = wg_hbm.shape[1]
    sends = s < n_section - 1
    owns = s > 0

    home = (0, 0)
    moves = sorted(
        ((dx, dl) for dx in range(chips) for dl in range(n_local)),
        key=lambda d: -min(d[0], chips - d[0]) - min(d[1], n_local - d[1]),
    )
    here = [d for d in moves if d[1] % 2 == 1]
    above = [d for d in moves if d not in here]
    waves = [[d for d in moves if (d[0] + d[1]) % 2 == odd] for odd in range(2)]
    waves = [[d for d in wave if d in here] + [d for d in wave if d in above] for wave in waves]
    slots = waves[0] + waves[1]

    def drain(held, sem):
        pltpu.make_async_copy(held, held, sem).wait()

    def span(group):
        low = slots.index(group[0]) * 2 * B
        return slice(low, low + len(group) * 2 * B)

    def place(move, side):
        return (n // 2 + move[0]) % chips * 2 + side, (l + move[1]) % n_local

    def back(move):
        return -move[0], -move[1]

    def cols(k):
        return pl.ds(k * piece, piece)

    tok_copies = [
        pltpu.make_async_copy(
            tok_hbm.at[:, cols(k)], tok.at[pl.ds(k * tok_pad, tok_dev)], tok_sem.at[k]
        )
        for k in range(G)
    ]
    w_copies = [
        pltpu.make_async_copy(
            hbm.at[pl.ds(i * hbm.shape[0] // SPLIT, hbm.shape[0] // SPLIT)],
            held.at[pl.ds(i * hbm.shape[0] // SPLIT, hbm.shape[0] // SPLIT)],
            w_sem.at[w * SPLIT + i],
        )
        for w, (hbm, held) in enumerate(((wg_hbm, wg), (wu_hbm, wu), (wd_hbm, wd)))
        for i in range(SPLIT)
    ]
    in_copies = [
        pltpu.make_async_copy(table_hbm, table_ref, in_sem.at[0]),
        pltpu.make_async_copy(routes_hbm, routes_ref, in_sem.at[1]),
        pltpu.make_async_copy(gates_hbm, gates_ref, in_sem.at[2]),
    ]

    barrier = pltpu.get_barrier_semaphore()

    def greet(section, move, side):
        j, m = place(move, side)
        pl.semaphore_signal(barrier, inc=1, device_id=(section, j, m), device_id_type=MESH)

    for move in moves:
        for flip in range(2):
            if move != home or flip:
                greet(s, move, core ^ flip)

    callers = [(home, flip) for flip in range(2)]

    @pl.when(owns)
    def _():
        for move, flip in callers:
            greet(s - 1, move, core ^ flip)

    @pl.when(sends)
    def _():
        greet(s + 1, home, core)

    for c in in_copies + tok_copies:
        c.start()
    for c in in_copies:
        c.wait()

    ids[...] = jnp.full(ids.shape, -1, jnp.int32)
    vals[...] = jnp.zeros(vals.shape, jnp.float32)
    ids[:, :tok_dev] = routes_ref[...]
    vals[:, :tok_dev] = gates_ref[...]
    picks = ids[...]
    gates = vals[...]
    named_rows = max(16, n_node)
    row_id = lax.broadcasted_iota(jnp.int32, (named_rows, tok_pad), 0)
    named = jnp.zeros((named_rows, tok_pad), jnp.float32)
    hits, weights = [], []
    for j in range(n_node):
        hit = picks == table_ref[j]
        hits.append(jnp.max(jnp.where(hit, 1.0, 0.0), axis=0, keepdims=True))
        weights.append(jnp.sum(jnp.where(hit, gates, 0.0), axis=0, keepdims=True))
        named = jnp.where(row_id == j, hits[j], named)
    before = lax.broadcasted_iota(jnp.int32, (tok_pad, tok_pad), 0) < lax.broadcasted_iota(
        jnp.int32, (tok_pad, tok_pad), 1
    )
    rank = jnp.dot(
        named.astype(jnp.bfloat16),
        jnp.where(before, 1.0, 0.0).astype(jnp.bfloat16),
        preferred_element_type=jnp.float32,
    ).astype(jnp.int32)
    chosen = []
    for j in range(n_node):
        copies = jnp.int32(0)
        replica = jnp.int32(0)
        for i in range(n_node):
            same = (table_ref[i] == table_ref[j]).astype(jnp.int32)
            copies = copies + same
            if i < j:
                replica = replica + same
        for p in range(CAP):
            want = p * copies + replica
            sel = jnp.where(rank[j : j + 1] == want, hits[j], 0.0)
            comb_own[j * CAP + p : j * CAP + p + 1, :] = sel * weights[j]
            chosen.append(jnp.broadcast_to(sel, (G, tok_pad)))
    chosen = jnp.concatenate(chosen, axis=0)
    piece_of = row_piece(chosen.shape)
    select = jnp.concatenate(
        [jnp.where(piece_of == k, chosen, 0.0).astype(jnp.bfloat16) for k in range(G)], axis=1
    )
    if tok_pad > tok_dev:
        for k in range(G):
            tok[k * tok_pad + tok_dev : (k + 1) * tok_pad, :] = jnp.zeros(
                (tok_pad - tok_dev, piece), jnp.bfloat16
            )
    for c in tok_copies:
        c.wait()
    for c in w_copies:
        c.start()
    def dispatch(move, side, low, high):
        j, m = place(move, side)
        wave = int(move in waves[1])
        up = int(move in above)
        return pltpu.make_async_remote_copy(
            src_ref=disp.at[pl.ds(pl.multiple_of(j * B, B), B), low:high],
            dst_ref=recv.at[block_of(move, core), low:high],
            send_sem=send_sem.at[wave],
            recv_sem=recv_sem.at[wave, up, low // IN],
            device_id=(s + up, j, m),
            device_id_type=MESH,
        )

    def block_of(move, side):
        return pl.ds(pl.multiple_of((slots.index(move) * 2 + side) * B, B), B)

    comb_copy = pltpu.make_async_remote_copy(
        src_ref=comb_own, dst_ref=comb_in, send_sem=comb_send.at[0], recv_sem=comb_recv.at[0],
        device_id=(s + 1, n, l), device_id_type=MESH,
    )
    for low, high in chunks(piece, IN):
        disp[:, low:high] = jnp.dot(
            select, tok[:, low:high], preferred_element_type=jnp.float32
        ).astype(jnp.bfloat16)
        if low == 0:
            pl.semaphore_wait(
                barrier,
                sources - 1
                + len(callers) * sends.astype(jnp.int32)
                + owns.astype(jnp.int32),
            )

        @pl.when(sends)
        def _():
            for move in waves[0]:
                for side in range(2):
                    dispatch(move, side, low, high).start()

    @pl.when(owns)
    def _():
        pl.semaphore_signal(up_sem, inc=1, device_id=(s - 1, n, l), device_id_type=MESH)

    @pl.when(sends)
    def _():
        comb_copy.start()
        for low, high in chunks(piece, IN):
            for move in waves[1]:
                if move in here:
                    for side in range(2):
                        dispatch(move, side, low, high).start()
        pl.semaphore_wait(up_sem, 1)
        for low, high in chunks(piece, IN):
            for move in waves[1]:
                if move in above:
                    for side in range(2):
                        dispatch(move, side, low, high).start()

    def give_back(move, side, low, high):
        qn, ql = place(back(move), side)
        up = int(move in here)
        return pltpu.make_async_remote_copy(
            src_ref=outb.at[block_of(move, side), low:high],
            dst_ref=ret.at[l, pl.ds(pl.multiple_of(n * B, B), B), low:high],
            send_sem=back_sem.at[up],
            recv_sem=ret_sem.at[0],
            device_id=(s + up, qn, ql),
            device_id_type=MESH,
        )

    for c in w_copies:
        c.wait()

    for number, wave in enumerate(waves):
        stay = [move for move in wave if move in here]
        rise = [move for move in wave if move in above]

        count = len(wave) * 2 * B
        piece_id = row_piece((count, 2 * hid))
        total = jnp.zeros((count, 2 * hid), jnp.float32)
        for low, high in chunks(piece, IN):

            @pl.when(sends)
            def _():
                drain(recv.at[span(stay), low:high], recv_sem.at[number, 0, low // IN])

            @pl.when(owns)
            def _():
                drain(recv.at[span(rise), low:high], recv_sem.at[number, 1, low // IN])

            rows = recv[span(wave), low:high]
            for k in range(G):
                cut = slice(k * piece + low, k * piece + high)
                both = jnp.concatenate([wg[cut, :], wu[cut, :]], axis=1)
                part = jnp.dot(rows, both, preferred_element_type=jnp.float32)
                total = total + jnp.where(piece_id == k, part, 0.0)
        total = total.reshape(count // G, G, 2 * hid)
        total = jnp.broadcast_to(jnp.sum(total, axis=1, keepdims=True), total.shape)
        total = total.reshape(count, 2 * hid)
        gate_proj = total[:, :hid]
        up_proj = total[:, hid:]
        hidden = gate_proj / (1.0 + jnp.exp(-gate_proj)) * up_proj
        piece_h = row_piece(hidden.shape)
        spread = jnp.concatenate(
            [jnp.where(piece_h == k, hidden, 0.0).astype(jnp.bfloat16) for k in range(G)],
            axis=1,
        )
        for low, high in chunks(piece, piece):
            down = jnp.concatenate(
                [wd[:, k * piece + low : k * piece + high] for k in range(G)], axis=0
            )
            outb[span(wave), low:high] = jnp.dot(
                spread, down, preferred_element_type=jnp.float32
            ).astype(jnp.bfloat16)

            @pl.when(sends)
            def _():
                for move in stay:
                    for side in range(2):
                        give_back(move, side, low, high).start()

            @pl.when(owns)
            def _():
                for move in rise:
                    if move != home:
                        for side in range(2):
                            give_back(move, side, low, high).start()
                    else:
                        give_back(move, 1 - core, low, high).start()
                        pltpu.make_async_copy(
                            outb.at[block_of(home, core), low:high],
                            ret.at[l, pl.ds(pl.multiple_of(n * B, B), B), low:high],
                            ret_sem.at[0],
                        ).start()

    @pl.when(owns)
    def _():
        comb_copy.wait_recv()
        mix = comb_in[...]
        high = mix.astype(jnp.bfloat16).astype(jnp.float32)
        tall = jnp.concatenate(
            [
                jnp.broadcast_to(part[c : c + 1], (G, tok_pad))
                for part in (high, mix - high)
                for c in range(n_node * CAP)
            ],
            axis=0,
        )
        mix_ref[...] = jnp.transpose(tall).astype(jnp.bfloat16)
        drain(ret, ret_sem.at[0])
        summed = ret[0].astype(jnp.float32)
        for m in range(1, n_local):
            summed = summed + ret[m].astype(jnp.float32)
        rows_ref[...] = summed.astype(jnp.bfloat16)

    @pl.when(s == 0)
    def _():
        rows_ref[...] = jnp.zeros(rows_ref.shape, jnp.bfloat16)
        mix_ref[...] = jnp.zeros(mix_ref.shape, jnp.bfloat16)

    @pl.when(sends)
    def _():
        drain(recv.at[span(waves[0])], send_sem.at[0])
        drain(recv.at[span(waves[1])], send_sem.at[1])
        drain(outb.at[: len(here) * 2 * B], back_sem.at[1])
        comb_copy.wait_send()

    @pl.when(owns)
    def _():
        drain(outb.at[: len(above) * 2 * B - B], back_sem.at[0])


def expand_kernel(rows_ref, mix_ref, out_hbm, obuf, sem):
    tok_dev = out_hbm.shape[0]
    piece = rows_ref.shape[1]
    rows = rows_ref[...]
    rows = jnp.concatenate([rows, rows], axis=0)
    mix = mix_ref[:tok_dev, :].astype(jnp.float32)
    lane = lax.broadcasted_iota(jnp.int32, mix.shape, 1) % G
    copies = []
    for k in range(G):
        left = jnp.where(lane == k, mix, 0.0).astype(jnp.bfloat16)
        obuf[k] = jnp.dot(left, rows, preferred_element_type=jnp.float32).astype(jnp.bfloat16)
        copy = pltpu.make_async_copy(
            obuf.at[k], out_hbm.at[:, pl.ds(k * piece, piece)], sem.at[k]
        )
        copy.start()
        copies.append(copy)
    for copy in copies:
        copy.wait()


def shards(n_section, tokens, routes, route_gates, replica_table, w_gate, w_up, w_down):
    n_node = lax.axis_size("node")
    n_local = lax.axis_size("local")
    sources = n_node * n_local
    tok_dev, width = tokens.shape[1:]
    topk = routes.shape[2]
    hid = w_gate.shape[2]
    piece = width // G
    tok_pad = -(-tok_dev // 128) * 128
    slots = n_node * CAP
    vmem = pl.BlockSpec(memory_space=pltpu.VMEM)
    hbm = pl.BlockSpec(memory_space=pltpu.HBM)
    rows, mix = pl.pallas_call(
        functools.partial(relay_kernel, n_section, n_node, n_local),
        out_shape=(
            pltpu.VMEM((n_node * B, piece), jnp.bfloat16),
            pltpu.VMEM((tok_pad, 2 * slots * G), jnp.bfloat16),
        ),
        in_specs=[hbm] * 7,
        out_specs=(vmem, vmem),
        scratch_shapes=[
            pltpu.SMEM((n_node,), jnp.int32),
            pltpu.VMEM((topk, tok_dev), jnp.int32),
            pltpu.VMEM((topk, tok_dev), jnp.float32),
            pltpu.VMEM((topk, tok_pad), jnp.int32),
            pltpu.VMEM((topk, tok_pad), jnp.float32),
            pltpu.VMEM((G * tok_pad, piece), jnp.bfloat16),
            pltpu.VMEM((width, hid), jnp.bfloat16),
            pltpu.VMEM((width, hid), jnp.bfloat16),
            pltpu.VMEM((hid, width), jnp.bfloat16),
            pltpu.VMEM((n_node * B, piece), jnp.bfloat16),
            pltpu.VMEM((sources * B, piece), jnp.bfloat16),
            pltpu.VMEM((sources * B, piece), jnp.bfloat16),
            pltpu.VMEM((n_local, n_node * B, piece), jnp.bfloat16),
            pltpu.VMEM((slots, tok_pad), jnp.float32),
            pltpu.VMEM((slots, tok_pad), jnp.float32),
            pltpu.SemaphoreType.DMA((3,)),
            pltpu.SemaphoreType.DMA((G,)),
            pltpu.SemaphoreType.DMA((3 * SPLIT,)),
            pltpu.SemaphoreType.DMA((2,)),
            pltpu.SemaphoreType.DMA((2, 2, len(chunks(piece, IN)))),
            pltpu.SemaphoreType.DMA((2,)),
            pltpu.SemaphoreType.DMA((1,)),
            pltpu.SemaphoreType.DMA((1,)),
            pltpu.SemaphoreType.DMA((1,)),
            pltpu.SemaphoreType.REGULAR,
        ],
        compiler_params=pltpu.CompilerParams(
            collective_id=0, has_side_effects=True, vmem_limit_bytes=KEEP
        ),
        name="relay",
    )(
        *(
            pltpu.with_memory_space_constraint(a, pltpu.HBM)
            for a in (
                replica_table,
                jnp.transpose(routes[0]),
                jnp.transpose(route_gates[0]),
                tokens[0],
                w_gate[0],
                w_up[0],
                w_down[0],
            )
        )
    )
    out = pl.pallas_call(
        expand_kernel,
        out_shape=jax.ShapeDtypeStruct((tok_dev, width), jnp.bfloat16),
        in_specs=[vmem, vmem],
        out_specs=hbm,
        scratch_shapes=[
            pltpu.VMEM((G, tok_dev, piece), jnp.bfloat16),
            pltpu.SemaphoreType.DMA((G,)),
        ],
        compiler_params=pltpu.CompilerParams(vmem_limit_bytes=KEEP),
        name="expand",
    )(rows, mix)
    return out[None]


def solution(mesh):
    placed = (
        P("section", ("node", "local"), None),
        P("section", ("node", "local"), None),
        P("section", ("node", "local"), None),
        P(),
        P("node", None, "local"),
        P("node", None, "local"),
        P("node", "local", None),
    )
    return jax.shard_map(
        functools.partial(shards, mesh.shape["section"]),
        mesh=mesh,
        in_specs=placed,
        out_specs=P("section", ("node", "local"), None),
        check_vma=False,
    )
```

```python
import functools

import jax
import jax.numpy as jnp
from jax import lax
from jax.experimental import pallas as pl
from jax.experimental.pallas import tpu as pltpu
from jax.sharding import PartitionSpec as P

CAP = 2
G = 8
B = CAP * G
KEEP = 24 * 1024 * 1024
SPLIT = 4
LANES = 512
MESH = pl.DeviceIdType.MESH


def row_piece(shape):
    return lax.broadcasted_iota(jnp.int32, shape, 0) % G


def chunks(piece, step):
    return [(low, min(low + step, piece)) for low in range(0, piece, step)]


def relay_kernel(
    n_section, n_node, n_local,
    table_hbm, routes_hbm, gates_hbm, tok_hbm, wg_hbm, wu_hbm, wd_hbm,
    rows_ref, mix_ref,
    table_ref, routes_ref, gates_ref, ids, vals, tok, wg, wu, wd, disp, recv, outb, ret, comb_own, comb_in,
    in_sem, tok_sem, w_sem, send_sem, recv_sem, back_sem, ret_sem, comb_send, comb_recv, up_sem,
):
    s = lax.axis_index("section")
    n = lax.axis_index("node")
    l = lax.axis_index("local")
    core = n % 2
    chips = n_node // 2
    sources = n_node * n_local
    tok_dev, width = tok_hbm.shape
    piece = width // G
    tok_pad = ids.shape[1]
    hid = wg_hbm.shape[1]
    sends = s < n_section - 1
    owns = s > 0

    home = (0, 0)
    moves = sorted(
        ((dx, dl) for dx in range(chips) for dl in range(n_local)),
        key=lambda d: -min(d[0], chips - d[0]) - min(d[1], n_local - d[1]),
    )
    here = [d for d in moves if d[1] % 2 == 1]
    above = [d for d in moves if d not in here]
    waves = [[d for d in moves if (d[0] + d[1]) % 2 == odd] for odd in range(2)]
    waves = [[d for d in wave if d in here] + [d for d in wave if d in above] for wave in waves]
    slots = waves[0] + waves[1]

    def drain(held, sem):
        pltpu.make_async_copy(held, held, sem).wait()

    def span(group):
        low = slots.index(group[0]) * 2 * B
        return slice(low, low + len(group) * 2 * B)

    def place(move, side):
        return (n // 2 + move[0]) % chips * 2 + side, (l + move[1]) % n_local

    def back(move):
        return -move[0], -move[1]

    def cols(k):
        return pl.ds(k * piece, piece)

    tok_copies = [
        pltpu.make_async_copy(
            tok_hbm.at[:, cols(k)], tok.at[pl.ds(k * tok_pad, tok_dev)], tok_sem.at[k]
        )
        for k in range(G)
    ]
    w_copies = [
        pltpu.make_async_copy(
            hbm.at[pl.ds(i * hbm.shape[0] // SPLIT, hbm.shape[0] // SPLIT)],
            held.at[pl.ds(i * hbm.shape[0] // SPLIT, hbm.shape[0] // SPLIT)],
            w_sem.at[w * SPLIT + i],
        )
        for w, (hbm, held) in enumerate(((wg_hbm, wg), (wu_hbm, wu), (wd_hbm, wd)))
        for i in range(SPLIT)
    ]
    in_copies = [
        pltpu.make_async_copy(table_hbm, table_ref, in_sem.at[0]),
        pltpu.make_async_copy(routes_hbm, routes_ref, in_sem.at[1]),
        pltpu.make_async_copy(gates_hbm, gates_ref, in_sem.at[2]),
    ]

    barrier = pltpu.get_barrier_semaphore()

    def greet(section, move, side):
        j, m = place(move, side)
        pl.semaphore_signal(barrier, inc=1, device_id=(section, j, m), device_id_type=MESH)

    for move in moves:
        for flip in range(2):
            if move != home or flip:
                greet(s, move, core ^ flip)

    callers = [(home, flip) for flip in range(2)]

    @pl.when(owns)
    def _():
        for move, flip in callers:
            greet(s - 1, move, core ^ flip)

    @pl.when(sends)
    def _():
        greet(s + 1, home, core)

    for c in in_copies + tok_copies:
        c.start()
    for c in in_copies:
        c.wait()

    ids[...] = jnp.full(ids.shape, -1, jnp.int32)
    vals[...] = jnp.zeros(vals.shape, jnp.float32)
    ids[:, :tok_dev] = routes_ref[...]
    vals[:, :tok_dev] = gates_ref[...]
    picks = ids[...]
    gates = vals[...]
    named_rows = max(16, n_node)
    row_id = lax.broadcasted_iota(jnp.int32, (named_rows, tok_pad), 0)
    named = jnp.zeros((named_rows, tok_pad), jnp.float32)
    hits, weights = [], []
    for j in range(n_node):
        hit = picks == table_ref[j]
        hits.append(jnp.max(jnp.where(hit, 1.0, 0.0), axis=0, keepdims=True))
        weights.append(jnp.sum(jnp.where(hit, gates, 0.0), axis=0, keepdims=True))
        named = jnp.where(row_id == j, hits[j], named)
    before = lax.broadcasted_iota(jnp.int32, (tok_pad, tok_pad), 0) < lax.broadcasted_iota(
        jnp.int32, (tok_pad, tok_pad), 1
    )
    rank = jnp.dot(
        named.astype(jnp.bfloat16),
        jnp.where(before, 1.0, 0.0).astype(jnp.bfloat16),
        preferred_element_type=jnp.float32,
    ).astype(jnp.int32)
    chosen = []
    for j in range(n_node):
        copies = jnp.int32(0)
        replica = jnp.int32(0)
        for i in range(n_node):
            same = (table_ref[i] == table_ref[j]).astype(jnp.int32)
            copies = copies + same
            if i < j:
                replica = replica + same
        for p in range(CAP):
            want = p * copies + replica
            sel = jnp.where(rank[j : j + 1] == want, hits[j], 0.0)
            comb_own[j * CAP + p : j * CAP + p + 1, :] = sel * weights[j]
            chosen.append(jnp.broadcast_to(sel, (G, tok_pad)))
    chosen = jnp.concatenate(chosen, axis=0)
    piece_of = row_piece(chosen.shape)
    select = jnp.concatenate(
        [jnp.where(piece_of == k, chosen, 0.0).astype(jnp.bfloat16) for k in range(G)], axis=1
    )
    if tok_pad > tok_dev:
        for k in range(G):
            tok[k * tok_pad + tok_dev : (k + 1) * tok_pad, :] = jnp.zeros(
                (tok_pad - tok_dev, piece), jnp.bfloat16
            )
    for c in tok_copies:
        c.wait()
    for c in w_copies:
        c.start()
    def dispatch(move, side, low, high):
        j, m = place(move, side)
        wave = int(move in waves[1])
        up = int(move in above)
        return pltpu.make_async_remote_copy(
            src_ref=disp.at[pl.ds(pl.multiple_of(j * B, B), B), low:high],
            dst_ref=recv.at[block_of(move, core), low:high],
            send_sem=send_sem.at[wave],
            recv_sem=recv_sem.at[wave, up, low // LANES],
            device_id=(s + up, j, m),
            device_id_type=MESH,
        )

    def block_of(move, side):
        return pl.ds(pl.multiple_of((slots.index(move) * 2 + side) * B, B), B)

    comb_copy = pltpu.make_async_remote_copy(
        src_ref=comb_own, dst_ref=comb_in, send_sem=comb_send.at[0], recv_sem=comb_recv.at[0],
        device_id=(s + 1, n, l), device_id_type=MESH,
    )
    for low, high in chunks(piece, LANES):
        disp[:, low:high] = jnp.dot(
            select, tok[:, low:high], preferred_element_type=jnp.float32
        ).astype(jnp.bfloat16)
        if low == 0:
            pl.semaphore_wait(
                barrier,
                sources - 1
                + len(callers) * sends.astype(jnp.int32)
                + owns.astype(jnp.int32),
            )

        @pl.when(sends)
        def _():
            for move in waves[0]:
                for side in range(2):
                    dispatch(move, side, low, high).start()

    @pl.when(owns)
    def _():
        pl.semaphore_signal(up_sem, inc=1, device_id=(s - 1, n, l), device_id_type=MESH)

    @pl.when(sends)
    def _():
        comb_copy.start()
        for low, high in chunks(piece, LANES):
            for move in waves[1]:
                if move in here:
                    for side in range(2):
                        dispatch(move, side, low, high).start()
        pl.semaphore_wait(up_sem, 1)
        for low, high in chunks(piece, LANES):
            for move in waves[1]:
                if move in above:
                    for side in range(2):
                        dispatch(move, side, low, high).start()

    def give_back(move, side, low, high):
        qn, ql = place(back(move), side)
        up = int(move in here)
        return pltpu.make_async_remote_copy(
            src_ref=outb.at[block_of(move, side), low:high],
            dst_ref=ret.at[l, pl.ds(pl.multiple_of(n * B, B), B), low:high],
            send_sem=back_sem.at[up],
            recv_sem=ret_sem.at[0],
            device_id=(s + up, qn, ql),
            device_id_type=MESH,
        )

    for c in w_copies:
        c.wait()

    for number, wave in enumerate(waves):
        stay = [move for move in wave if move in here]
        rise = [move for move in wave if move in above]

        count = len(wave) * 2 * B
        piece_id = row_piece((count, 2 * hid))
        total = jnp.zeros((count, 2 * hid), jnp.float32)
        for low, high in chunks(piece, LANES):

            @pl.when(sends)
            def _():
                drain(recv.at[span(stay), low:high], recv_sem.at[number, 0, low // LANES])

            @pl.when(owns)
            def _():
                drain(recv.at[span(rise), low:high], recv_sem.at[number, 1, low // LANES])

            rows = recv[span(wave), low:high]
            for k in range(G):
                cut = slice(k * piece + low, k * piece + high)
                both = jnp.concatenate([wg[cut, :], wu[cut, :]], axis=1)
                part = jnp.dot(rows, both, preferred_element_type=jnp.float32)
                total = total + jnp.where(piece_id == k, part, 0.0)
        total = total.reshape(count // G, G, 2 * hid)
        total = jnp.broadcast_to(jnp.sum(total, axis=1, keepdims=True), total.shape)
        total = total.reshape(count, 2 * hid)
        gate_proj = total[:, :hid]
        up_proj = total[:, hid:]
        hidden = gate_proj / (1.0 + jnp.exp(-gate_proj)) * up_proj
        piece_h = row_piece(hidden.shape)
        spread = jnp.concatenate(
            [jnp.where(piece_h == k, hidden, 0.0).astype(jnp.bfloat16) for k in range(G)],
            axis=1,
        )
        for low, high in chunks(piece, LANES):
            down = jnp.concatenate(
                [wd[:, k * piece + low : k * piece + high] for k in range(G)], axis=0
            )
            outb[span(wave), low:high] = jnp.dot(
                spread, down, preferred_element_type=jnp.float32
            ).astype(jnp.bfloat16)

            @pl.when(sends)
            def _():
                for move in stay:
                    for side in range(2):
                        give_back(move, side, low, high).start()

            @pl.when(owns)
            def _():
                for move in rise:
                    if move != home:
                        for side in range(2):
                            give_back(move, side, low, high).start()
                    else:
                        give_back(move, 1 - core, low, high).start()
                        pltpu.make_async_copy(
                            outb.at[block_of(home, core), low:high],
                            ret.at[l, pl.ds(pl.multiple_of(n * B, B), B), low:high],
                            ret_sem.at[0],
                        ).start()

    @pl.when(owns)
    def _():
        comb_copy.wait_recv()
        mix = comb_in[...]
        high = mix.astype(jnp.bfloat16).astype(jnp.float32)
        tall = jnp.concatenate(
            [
                jnp.broadcast_to(part[c : c + 1], (G, tok_pad))
                for part in (high, mix - high)
                for c in range(n_node * CAP)
            ],
            axis=0,
        )
        mix_ref[...] = jnp.transpose(tall).astype(jnp.bfloat16)
        drain(ret, ret_sem.at[0])
        summed = ret[0].astype(jnp.float32)
        for m in range(1, n_local):
            summed = summed + ret[m].astype(jnp.float32)
        rows_ref[...] = summed.astype(jnp.bfloat16)

    @pl.when(s == 0)
    def _():
        rows_ref[...] = jnp.zeros(rows_ref.shape, jnp.bfloat16)
        mix_ref[...] = jnp.zeros(mix_ref.shape, jnp.bfloat16)

    @pl.when(sends)
    def _():
        drain(recv.at[span(waves[0])], send_sem.at[0])
        drain(recv.at[span(waves[1])], send_sem.at[1])
        drain(outb.at[: len(here) * 2 * B], back_sem.at[1])
        comb_copy.wait_send()

    @pl.when(owns)
    def _():
        drain(outb.at[: len(above) * 2 * B - B], back_sem.at[0])


def expand_kernel(rows_ref, mix_ref, out_hbm, obuf, sem):
    tok_dev = out_hbm.shape[0]
    piece = rows_ref.shape[1]
    rows = rows_ref[...]
    rows = jnp.concatenate([rows, rows], axis=0)
    mix = mix_ref[:tok_dev, :].astype(jnp.float32)
    lane = lax.broadcasted_iota(jnp.int32, mix.shape, 1) % G
    copies = []
    for k in range(G):
        left = jnp.where(lane == k, mix, 0.0).astype(jnp.bfloat16)
        obuf[k] = jnp.dot(left, rows, preferred_element_type=jnp.float32).astype(jnp.bfloat16)
        copy = pltpu.make_async_copy(
            obuf.at[k], out_hbm.at[:, pl.ds(k * piece, piece)], sem.at[k]
        )
        copy.start()
        copies.append(copy)
    for copy in copies:
        copy.wait()


def shards(n_section, tokens, routes, route_gates, replica_table, w_gate, w_up, w_down):
    n_node = lax.axis_size("node")
    n_local = lax.axis_size("local")
    sources = n_node * n_local
    tok_dev, width = tokens.shape[1:]
    topk = routes.shape[2]
    hid = w_gate.shape[2]
    piece = width // G
    tok_pad = -(-tok_dev // 128) * 128
    slots = n_node * CAP
    vmem = pl.BlockSpec(memory_space=pltpu.VMEM)
    hbm = pl.BlockSpec(memory_space=pltpu.HBM)
    rows, mix = pl.pallas_call(
        functools.partial(relay_kernel, n_section, n_node, n_local),
        out_shape=(
            pltpu.VMEM((n_node * B, piece), jnp.bfloat16),
            pltpu.VMEM((tok_pad, 2 * slots * G), jnp.bfloat16),
        ),
        in_specs=[hbm] * 7,
        out_specs=(vmem, vmem),
        scratch_shapes=[
            pltpu.SMEM((n_node,), jnp.int32),
            pltpu.VMEM((topk, tok_dev), jnp.int32),
            pltpu.VMEM((topk, tok_dev), jnp.float32),
            pltpu.VMEM((topk, tok_pad), jnp.int32),
            pltpu.VMEM((topk, tok_pad), jnp.float32),
            pltpu.VMEM((G * tok_pad, piece), jnp.bfloat16),
            pltpu.VMEM((width, hid), jnp.bfloat16),
            pltpu.VMEM((width, hid), jnp.bfloat16),
            pltpu.VMEM((hid, width), jnp.bfloat16),
            pltpu.VMEM((n_node * B, piece), jnp.bfloat16),
            pltpu.VMEM((sources * B, piece), jnp.bfloat16),
            pltpu.VMEM((sources * B, piece), jnp.bfloat16),
            pltpu.VMEM((n_local, n_node * B, piece), jnp.bfloat16),
            pltpu.VMEM((slots, tok_pad), jnp.float32),
            pltpu.VMEM((slots, tok_pad), jnp.float32),
            pltpu.SemaphoreType.DMA((3,)),
            pltpu.SemaphoreType.DMA((G,)),
            pltpu.SemaphoreType.DMA((3 * SPLIT,)),
            pltpu.SemaphoreType.DMA((2,)),
            pltpu.SemaphoreType.DMA((2, 2, len(chunks(piece, LANES)))),
            pltpu.SemaphoreType.DMA((2,)),
            pltpu.SemaphoreType.DMA((1,)),
            pltpu.SemaphoreType.DMA((1,)),
            pltpu.SemaphoreType.DMA((1,)),
            pltpu.SemaphoreType.REGULAR,
        ],
        compiler_params=pltpu.CompilerParams(
            collective_id=0, has_side_effects=True, vmem_limit_bytes=KEEP
        ),
        name="relay",
    )(
        *(
            pltpu.with_memory_space_constraint(a, pltpu.HBM)
            for a in (
                replica_table,
                jnp.transpose(routes[0]),
                jnp.transpose(route_gates[0]),
                tokens[0],
                w_gate[0],
                w_up[0],
                w_down[0],
            )
        )
    )
    out = pl.pallas_call(
        expand_kernel,
        out_shape=jax.ShapeDtypeStruct((tok_dev, width), jnp.bfloat16),
        in_specs=[vmem, vmem],
        out_specs=hbm,
        scratch_shapes=[
            pltpu.VMEM((G, tok_dev, piece), jnp.bfloat16),
            pltpu.SemaphoreType.DMA((G,)),
        ],
        compiler_params=pltpu.CompilerParams(vmem_limit_bytes=KEEP),
        name="expand",
    )(rows, mix)
    return out[None]


def solution(mesh):
    placed = (
        P("section", ("node", "local"), None),
        P("section", ("node", "local"), None),
        P("section", ("node", "local"), None),
        P(),
        P("node", None, "local"),
        P("node", None, "local"),
        P("node", "local", None),
    )
    return jax.shard_map(
        functools.partial(shards, mesh.shape["section"]),
        mesh=mesh,
        in_specs=placed,
        out_specs=P("section", ("node", "local"), None),
        check_vma=False,
    )
```
